256 devices in a mesh: expert: 8 (over y, core), shard: 32 (over z, x).
Axes of the slice: x: 4, y: 4, z: 8, core: 2. Of those that a mesh axis runs over, the one named last changes fastest.
Arguments:
- master_down: float32 [16, 6400, 4096], P('expert', None, 'shard'), may hold values from -0.15625 to 0.15625
- second_down: bfloat16 [16, 6400, 4096], P('expert', None, 'shard'), may hold values from -0.0390625 to 0.0390625
- router_weight: float32 [4096, 16], P('shard', 'expert'), may hold values from -0.09375 to 0.09375
- router_gain: float32 [4096], P('shard'), may hold values from 0.25 to 1.75
Outputs:
- final_down: bfloat16 [16, 6400, 4096], P('expert', 'shard')
- scale_down: float32 [16, 6400], P('expert', 'shard')
- serve_router: bfloat16 [4096, 16], replicated
The draws below stay inside these ranges and needn't reach their ends.
All inputs are finite; a program needn't handle non-finite values.
Results may differ from the reference program's by a relative error of at most 0.0085.
Values may be sent and summed in bfloat16 or wider, within the bound.
A program may use at most 64 MiB of HBM per device.

```python
import jax
import jax.numpy as jnp
from jax import lax

EXPERTS = 16
D_MODEL = 4096
D_EXPERT = 6400


def strengthened(values, own_key, source, target, shards_of, factor):
    def block_of(position):
        return (jnp.arange(values.shape[position]) // (values.shape[position] // shards_of)).reshape((-1,) + (1,) * (values.ndim - 1 - position))

    one_side = jax.random.permutation(own_key, shards_of)[block_of(target)]
    other_side = (block_of(target) + shards_of // 2) % shards_of
    return jnp.where((block_of(source) == one_side) | (block_of(source) == other_side), factor * values, values)


def steps_of(rng, dims, pieces, low, high):
    gain, own = 1.0, jax.random.fold_in(rng, 6)
    for axis_at, parts in pieces:
        steps = jnp.exp(jax.random.uniform(jax.random.fold_in(own, axis_at), (parts,), jnp.float32, low / len(pieces), high / len(pieces)))
        gain = gain * jnp.repeat(steps, dims[axis_at] // parts).reshape([-1 if axis == axis_at else 1 for axis in range(len(dims))])
    return gain


def gaussian(own_key, shape, scale, reach, cuts=(), held_as=jnp.bfloat16):
    level = steps_of(own_key, shape, cuts, -0.22, 0.18) if cuts else 1.0
    values = jax.random.normal(own_key, shape, jnp.float32) * scale * level
    return jnp.minimum(jnp.maximum(values, -reach), reach).astype(held_as)


def bell_draw_with(stream_key, shape, deviation, most, cuts, heavy, held_as=jnp.bfloat16):
    drawn = deviation * jax.random.normal(stream_key, shape, jnp.float32)
    if cuts:
        drawn = drawn * steps_of(stream_key, shape, cuts, -0.22, 0.18)
    return jnp.clip(strengthened(drawn, jax.random.fold_in(stream_key, 3), *heavy), -most, most).astype(held_as)


def setup_inputs(seed: int = 0) -> dict:
    key_list = jax.random.split(jax.random.key(seed), 5)
    master_down = bell_draw_with(key_list[0], (EXPERTS, D_EXPERT, D_MODEL), D_EXPERT ** -0.5, 0.15625, ((0, 8), (2, 32)), (2, 1, 32, 2.75), jnp.float32)
    second_down = gaussian(key_list[1], (EXPERTS, D_EXPERT, D_MODEL), (D_EXPERT * 4) ** -0.5, 0.0390625, ((0, 8), (2, 32)))
    router_weight = gaussian(key_list[2], (D_MODEL, EXPERTS), D_MODEL ** -0.5, 0.09375, ((0, 32), (1, 8)), jnp.float32)
    router_gain = jnp.clip(1.0 + 0.15 * jax.random.normal(key_list[3], (D_MODEL,), jnp.float32), 0.25, 1.75)
    return {"master_down": master_down, "second_down": second_down, "router_weight": router_weight, "router_gain": router_gain}


def reference(master_down, second_down, router_weight, router_gain):
    merged_down = master_down + second_down.astype(jnp.float32)
    scale_down = jnp.sqrt(lax.optimization_barrier(jnp.sum(merged_down * merged_down, axis=2)))
    final_down = (merged_down / jnp.expand_dims(scale_down, 2)).astype(jnp.bfloat16)
    serve_router = (router_weight * router_gain[:, None]).astype(jnp.bfloat16)
    return (final_down, scale_down, serve_router)
```

```python
import jax
import jax.numpy as jnp
from jax import lax
from jax.sharding import PartitionSpec as P


def sent_to_all(x, axis):
    count = lax.axis_size(axis)
    return lax.all_to_all(jnp.broadcast_to(x[None], (count, *x.shape)), axis, 0, 0, tiled=True)


def body(master_down, second_down, router_weight, router_gain):
    shards = lax.axis_size("shard")
    experts, rows, width = master_down.shape
    merged = (master_down + second_down.astype(jnp.float32)).astype(jnp.bfloat16)
    parts = jnp.moveaxis(merged.reshape(experts, shards, rows // shards, width), 1, 0)
    mine = lax.all_to_all(parts, "shard", 0, 0, tiled=True).astype(jnp.float32)
    scale = jnp.sqrt(jnp.sum(mine * mine, axis=(0, 3)))
    final = (mine / scale[None, :, :, None]).astype(jnp.bfloat16)
    final = jnp.moveaxis(final, 0, 2).reshape(experts, rows // shards, shards * width)

    part_router = (router_weight * router_gain[:, None]).astype(jnp.bfloat16).T
    of_shards = sent_to_all(part_router, "shard")
    of_all = sent_to_all(of_shards, "expert")
    serve_router = jnp.transpose(of_all, (1, 3, 0, 2)).reshape(shards * width, -1)
    return (final, scale, serve_router)


def solution(mesh):
    placed = (
        P("expert", None, "shard"),
        P("expert", None, "shard"),
        P("shard", "expert"),
        P("shard"),
    )
    return jax.shard_map(
        body,
        mesh=mesh,
        in_specs=placed,
        out_specs=(P("expert", "shard", None), P("expert", "shard"), P()),
        check_vma=False,
    )
```

```python
import functools
import jax
import jax.numpy as jnp
from jax import lax
from jax.experimental import pallas as pl
from jax.experimental.pallas import tpu as pltpu
from jax.sharding import PartitionSpec as P

MESH = pl.DeviceIdType.MESH
LONG, WIDE = 8, 4
VLIM = 50 << 20
GROUP = 4


def offsets():
    near = lambda step, size: min(step, size - step)
    order = [(along, across) for along in range(LONG) for across in range(WIDE) if (along, across) != (0, 0)]
    return sorted(order, key=lambda s: (near(s[0], LONG) + near(s[1], WIDE), -near(s[0], LONG), s[1], s[0]))


def distance(step):
    return min(step[0], LONG - step[0]) + min(step[1], WIDE - step[1])


def exchange_kernel(order, experts, master, second, weight, gain, blocks, squares, routed,
                    router, wide, narrow, outgoing, in_sem, send_sem, recv_sem, along_sem, across_sem, expert_sem, round_sem):
    me, mine = lax.axis_index("shard"), lax.axis_index("expert")
    z, x = me // WIDE, lax.rem(me, WIDE)
    count = len(order)

    def shard_at(along, across):
        return lax.rem(z + along, LONG) * WIDE + lax.rem(x + across, WIDE)

    def peer(step):
        return shard_at(*order[step])

    def source(step):
        along, across = order[step]
        return shard_at((LONG - along) % LONG, (WIDE - across) % WIDE)

    def other(step):
        return lax.rem(mine + step + 1, experts)

    barrier = pltpu.get_barrier_semaphore()
    for step in range(count):
        pl.semaphore_signal(barrier, inc=1, device_id={"shard": peer(step)}, device_id_type=MESH)
    for step in range(experts - 1):
        pl.semaphore_signal(barrier, inc=1, device_id={"expert": other(step)}, device_id_type=MESH)

    def load(step):
        whom = peer(step) if step < count else me
        return (pltpu.make_async_copy(master.at[:, whom], wide.at[step], in_sem.at[step, 0]),
                pltpu.make_async_copy(second.at[:, whom], narrow.at[step], in_sem.at[step, 1]))

    def send(step, landing):
        return pltpu.make_async_remote_copy(
            src_ref=outgoing.at[step], dst_ref=blocks.at[landing], send_sem=send_sem.at[step],
            recv_sem=recv_sem.at[step], device_id={"shard": peer(step)}, device_id_type=MESH)

    def merge(step):
        for copy in load(step):
            copy.wait()
        return (wide[step] + narrow[step].astype(jnp.float32)).astype(jnp.bfloat16)

    def along_copy(step, landing):
        return pltpu.make_async_remote_copy(
            src_ref=router.at[mine, z, x], dst_ref=router.at[mine, landing, x], send_sem=along_sem.at[step, 0],
            recv_sem=along_sem.at[step, 1], device_id={"shard": shard_at(step + 1, 0)}, device_id_type=MESH)

    def across_copy(step, landing):
        return pltpu.make_async_remote_copy(
            src_ref=router.at[mine, :, x], dst_ref=router.at[mine, :, landing], send_sem=across_sem.at[step, 0],
            recv_sem=across_sem.at[step, 1], device_id={"shard": shard_at(0, step + 1)}, device_id_type=MESH)

    def expert_copy(step, landing):
        return pltpu.make_async_remote_copy(
            src_ref=router.at[mine], dst_ref=router.at[landing], send_sem=expert_sem.at[step, 0],
            recv_sem=expert_sem.at[step, 1], device_id={"expert": other(step)}, device_id_type=MESH)

    def before(index, step, size):
        return lax.rem(index + size - step - 1, size)

    for step in range(count + 1):
        for copy in load(step):
            copy.start()
    router[mine, z, x] = (weight[...] * gain[...]).astype(jnp.bfloat16)
    first = 4
    for step in range(first):
        outgoing[step] = merge(step)

    pl.semaphore_wait(barrier, count + experts - 1)

    for step in range(LONG - 1):
        along_copy(step, z).start()
    for step in range(first):
        send(step, me).start()
    for step in range(first, 13):
        outgoing[step] = merge(step)
    for step in range(first, 13):
        send(step, me).start()
    for step in range(13, count):
        outgoing[step] = merge(step)
    for step in range(LONG - 1):
        along_copy(step, before(z, step, LONG)).wait_recv()
    for step in range(WIDE - 1):
        across_copy(step, x).start()
    for step in range(13, count):
        send(step, me).start()
    own = merge(count)
    blocks[me] = own
    own = own.astype(jnp.float32)
    squares[...] = own * own
    for step in range(WIDE - 1):
        across_copy(step, before(x, step, WIDE)).wait_recv()
    for step in range(experts - 1):
        expert_copy(step, mine).start()

    for step in range(count):
        if step == count // 2:
            for turn in range(experts - 1):
                expert_copy(turn, before(mine, turn, experts)).wait_recv()
            for along in range(LONG):
                for across in range(WIDE):
                    start = (along * WIDE + across) * 128
                    routed[:, start:start + 128] = router[:, along, across].astype(jnp.float32).reshape(routed.shape[0], 128).astype(jnp.bfloat16)
        send(step, source(step)).wait_recv()
        part = blocks[source(step)].astype(jnp.float32)
        squares[...] += part * part

    for step in range(count):
        send(step, me).wait_send()
    for step in range(LONG - 1):
        along_copy(step, z).wait_send()
    for step in range(WIDE - 1):
        across_copy(step, x).wait_send()
    for step in range(experts - 1):
        expert_copy(step, mine).wait_send()


def exchange(master, second, weight, gain, order):
    held, shards, rows, width = master.shape
    experts = lax.axis_size("expert")
    count = len(order)
    vmem, hbm = pl.BlockSpec(memory_space=pltpu.VMEM), pl.BlockSpec(memory_space=pltpu.MemorySpace.HBM)
    dma = pltpu.SemaphoreType.DMA
    return pl.pallas_call(
        functools.partial(exchange_kernel, order, experts),
        out_shape=(
            jax.ShapeDtypeStruct((shards, held, rows, width), jnp.bfloat16),
            jax.ShapeDtypeStruct((held, rows, width), jnp.float32),
            jax.ShapeDtypeStruct((experts * held, shards * width), jnp.bfloat16),
        ),
        in_specs=[hbm, hbm, vmem, vmem],
        out_specs=(vmem, vmem, vmem),
        scratch_shapes=[
            pltpu.VMEM((experts, LONG, WIDE, held, width), jnp.bfloat16),
            pltpu.VMEM((shards, held, rows, width), jnp.float32),
            pltpu.VMEM((shards, held, rows, width), jnp.bfloat16),
            pltpu.VMEM((count, held, rows, width), jnp.bfloat16),
            dma((shards, 2)), dma((count,)), dma((count,)), dma((LONG - 1, 2)), dma((WIDE - 1, 2)),
            dma((experts - 1, 2)), pltpu.SemaphoreType.REGULAR((8,)),
        ],
        compiler_params=pltpu.CompilerParams(collective_id=0, has_side_effects=True, vmem_limit_bytes=VLIM),
    )(master, second, weight, gain)


def finish_kernel(blocks, squares, routed, final, scale, serve, ready, sem):
    held, rows, width = squares.shape
    copies = [pltpu.make_async_copy(routed, serve, sem.at[0])]
    copies[0].start()
    by_lane = jnp.stack([jnp.sum(jnp.swapaxes(squares[e], 0, 1), axis=0) for e in range(held)])
    scale[...] = jnp.sqrt(by_lane)
    inverse = [1.0 / jnp.sqrt(jnp.sum(squares[e], axis=1, keepdims=True)) for e in range(held)]
    for e in range(held):
        squares[e] = jnp.broadcast_to(inverse[e], (rows, width))
    for start in range(0, blocks.shape[0], GROUP):
        for shard in range(start, start + GROUP):
            ready[:, :, shard * width:(shard + 1) * width] = (
                blocks[shard].astype(jnp.float32) * squares[...]).astype(jnp.bfloat16)
        lanes = pl.ds(start * width, GROUP * width)
        copies.append(pltpu.make_async_copy(ready.at[:, :, lanes], final.at[:, :, lanes], sem.at[len(copies)]))
        copies[-1].start()
    for copy in copies:
        copy.wait()


def finish(blocks, squares, routed):
    shards, held, rows, width = blocks.shape
    vmem, hbm = pl.BlockSpec(memory_space=pltpu.VMEM), pl.BlockSpec(memory_space=pl.ANY)
    return pl.pallas_call(
        finish_kernel,
        out_shape=(
            jax.ShapeDtypeStruct((held, rows, shards * width), jnp.bfloat16),
            jax.ShapeDtypeStruct((held, rows), jnp.float32),
            jax.ShapeDtypeStruct(routed.shape, jnp.bfloat16),
        ),
        in_specs=[vmem, vmem, vmem],
        out_specs=(hbm, vmem, hbm),
        scratch_shapes=[
            pltpu.VMEM((held, rows, shards * width), jnp.bfloat16),
            pltpu.SemaphoreType.DMA((1 + shards // GROUP,)),
        ],
        compiler_params=pltpu.CompilerParams(vmem_limit_bytes=VLIM),
    )(blocks, squares, routed)


def body(master_down, second_down, router_weight, router_gain):
    shards = lax.axis_size("shard")
    held, rows, width = master_down.shape
    cut = (held, shards, rows // shards, width)
    gathered = exchange(
        master_down.reshape(cut), second_down.reshape(cut), router_weight.T, router_gain[None, :], offsets())
    final, scale, serve_router = finish(*gathered)
    return (final, scale, serve_router.T)


def solution(mesh):
    placed = (
        P("expert", None, "shard"),
        P("expert", None, "shard"),
        P("shard", "expert"),
        P("shard"),
    )
    return jax.shard_map(
        body,
        mesh=mesh,
        in_specs=placed,
        out_specs=(P("expert", "shard", None), P("expert", "shard"), P()),
        check_vma=False,
    )
```

```python
import functools
import jax
import jax.numpy as jnp
from jax import lax
from jax.experimental import pallas as pl
from jax.experimental.pallas import tpu as pltpu
from jax.sharding import PartitionSpec as P

MESH = pl.DeviceIdType.MESH
LONG, WIDE = 8, 4
VLIM = 50 << 20
GROUP = 4
ROUNDS = LONG // 2 + WIDE // 2 - 1


def plan():
    near = lambda step, size: min(step, size - step)
    early = [[(1, 0), (LONG - 1, 0), (0, 1), (0, WIDE - 1)], [(2, 0), (LONG - 2, 0)], [(3, 0), (LONG - 3, 0)]]
    used = [step for group in early for step in group] + [(0, 0)]
    rest = [(along, across) for along in range(LONG) for across in range(WIDE) if (along, across) not in used]
    rest.sort(key=lambda s: (-near(s[0], LONG) - near(s[1], WIDE), -near(s[0], LONG), s[1], s[0]))
    return early + [[]] * (ROUNDS - len(early)) + [rest]


def exchange_kernel(plan, experts, master, second, part, blocks, squares, routed,
                    router, wide, narrow, outgoing, in_sem, send_sem, recv_sem, along_sem, across_sem, expert_sem, round_sem):
    me, mine = lax.axis_index("shard"), lax.axis_index("expert")
    z, x = me // WIDE, lax.rem(me, WIDE)
    order = [step for group in plan for step in group]
    count = len(order)

    def shard_at(along, across):
        return lax.rem(z + along, LONG) * WIDE + lax.rem(x + across, WIDE)

    def peer(step):
        return shard_at(*order[step])

    def source(step):
        along, across = order[step]
        return shard_at((LONG - along) % LONG, (WIDE - across) % WIDE)

    def other(step):
        return lax.rem(mine + step + 1, experts)

    def greet(turn):
        semaphore = pltpu.get_barrier_semaphore() if turn == 1 else round_sem.at[turn - 2]
        for along, across in ((1, 0), (LONG - 1, 0), (0, 1), (0, WIDE - 1)):
            pl.semaphore_signal(semaphore, inc=1, device_id={"shard": shard_at(along, across)}, device_id_type=MESH)
        if turn <= 3:
            for near in around:
                pl.semaphore_signal(semaphore, inc=1, device_id={"expert": near}, device_id_type=MESH)

    def greeted(turn):
        semaphore = pltpu.get_barrier_semaphore() if turn == 1 else round_sem.at[turn - 2]
        pl.semaphore_wait(semaphore, 7 if turn <= 3 else 4)

    around = (mine + 1 - 2 * lax.rem(mine, 2), lax.rem(mine + 2, experts), lax.rem(mine + experts - 2, experts))
    greet(1)

    def load(step):
        whom = peer(step) if step < count else me
        return (pltpu.make_async_copy(master.at[:, whom], wide.at[step], in_sem.at[step, 0]),
                pltpu.make_async_copy(second.at[:, whom], narrow.at[step], in_sem.at[step, 1]))

    def send(step, landing):
        return pltpu.make_async_remote_copy(
            src_ref=outgoing.at[step], dst_ref=blocks.at[landing], send_sem=send_sem.at[step],
            recv_sem=recv_sem.at[step], device_id={"shard": peer(step)}, device_id_type=MESH)

    def merge(step):
        for copy in load(step):
            copy.wait()
        return (wide[step] + narrow[step].astype(jnp.float32)).astype(jnp.bfloat16)

    def along_copy(step, landing):
        return pltpu.make_async_remote_copy(
            src_ref=router.at[mine, z, x], dst_ref=router.at[mine, landing, x], send_sem=along_sem.at[step, 0],
            recv_sem=along_sem.at[step, 1], device_id={"shard": shard_at(step + 1, 0)}, device_id_type=MESH)

    def across_copy(step, landing):
        return pltpu.make_async_remote_copy(
            src_ref=router.at[mine, :, x], dst_ref=router.at[mine, :, landing], send_sem=across_sem.at[step, 0],
            recv_sem=across_sem.at[step, 1], device_id={"shard": shard_at(0, step + 1)}, device_id_type=MESH)

    def expert_copy(step, landing):
        return pltpu.make_async_remote_copy(
            src_ref=router.at[mine], dst_ref=router.at[landing], send_sem=expert_sem.at[step, 0],
            recv_sem=expert_sem.at[step, 1], device_id={"expert": other(step)}, device_id_type=MESH)

    def before(index, step, size):
        return lax.rem(index + size - step - 1, size)

    for step in range(count + 1):
        for copy in load(step):
            copy.start()

    bounds = [sum(len(group) for group in plan[:turn]) for turn in range(ROUNDS + 2)]
    for step in range(bounds[1]):
        outgoing[step] = merge(step)
    for turn in range(1, ROUNDS + 2):
        greeted(turn)
        if turn <= ROUNDS:
            greet(turn + 1)
        if turn == LONG // 2:
            for step in range(LONG - 1):
                along_copy(step, z).start()
        for step in range(bounds[turn - 1], bounds[turn]):
            send(step, me).start()
        if turn == 1:
            router[mine, z, x] = part[...]
        if turn <= ROUNDS:
            for step in range(bounds[turn], bounds[turn + 1]):
                outgoing[step] = merge(step)
    for step in range(LONG - 1):
        along_copy(step, before(z, step, LONG)).wait_recv()
    for step in range(WIDE - 1):
        across_copy(step, x).start()
    own = merge(count)
    blocks[me] = own
    own = own.astype(jnp.float32)
    squares[...] = own * own
    for step in range(WIDE - 1):
        across_copy(step, before(x, step, WIDE)).wait_recv()
    for step in range(experts - 1):
        expert_copy(step, mine).start()

    for step in range(count):
        if step == count // 2:
            for turn in range(experts - 1):
                expert_copy(turn, before(mine, turn, experts)).wait_recv()
            for along in range(LONG):
                for across in range(WIDE):
                    start = (along * WIDE + across) * 128
                    routed[:, start:start + 128] = router[:, along, across].astype(jnp.float32).reshape(routed.shape[0], 128).astype(jnp.bfloat16)
        send(step, source(step)).wait_recv()
        part = blocks[source(step)].astype(jnp.float32)
        squares[...] += part * part

    for step in range(count):
        send(step, me).wait_send()
    for step in range(LONG - 1):
        along_copy(step, z).wait_send()
    for step in range(WIDE - 1):
        across_copy(step, x).wait_send()
    for step in range(experts - 1):
        expert_copy(step, mine).wait_send()


def exchange(master, second, part, plan):
    held, shards, rows, width = master.shape
    experts = lax.axis_size("expert")
    count = shards - 1
    vmem, hbm = pl.BlockSpec(memory_space=pltpu.VMEM), pl.BlockSpec(memory_space=pltpu.MemorySpace.HBM)
    dma = pltpu.SemaphoreType.DMA
    return pl.pallas_call(
        functools.partial(exchange_kernel, plan, experts),
        out_shape=(
            jax.ShapeDtypeStruct((shards, held, rows, width), jnp.bfloat16),
            jax.ShapeDtypeStruct((held, rows, width), jnp.float32),
            jax.ShapeDtypeStruct((experts * held, shards * width), jnp.bfloat16),
        ),
        in_specs=[hbm, hbm, vmem],
        out_specs=(vmem, vmem, vmem),
        scratch_shapes=[
            pltpu.VMEM((experts, LONG, WIDE, held, width), jnp.bfloat16),
            pltpu.VMEM((shards, held, rows, width), jnp.float32),
            pltpu.VMEM((shards, held, rows, width), jnp.bfloat16),
            pltpu.VMEM((count, held, rows, width), jnp.bfloat16),
            dma((shards, 2)), dma((count,)), dma((count,)), dma((LONG - 1, 2)), dma((WIDE - 1, 2)),
            dma((experts - 1, 2)), pltpu.SemaphoreType.REGULAR((ROUNDS,)),
        ],
        compiler_params=pltpu.CompilerParams(collective_id=0, has_side_effects=True, vmem_limit_bytes=VLIM),
    )(master, second, part)


def finish_kernel(blocks, squares, routed, final, scale, serve, ready, inverse, sem):
    held, rows, width = squares.shape
    copies = [pltpu.make_async_copy(routed, serve, sem.at[0])]
    copies[0].start()
    for e in range(held):
        inverse[e] = jnp.broadcast_to(1.0 / jnp.sqrt(jnp.sum(squares[e], axis=1, keepdims=True)), (rows, width))
    for start in range(0, blocks.shape[0], GROUP):
        for shard in range(start, start + GROUP):
            ready[:, :, shard * width:(shard + 1) * width] = (
                blocks[shard].astype(jnp.float32) * inverse[...]).astype(jnp.bfloat16)
        lanes = pl.ds(start * width, GROUP * width)
        copies.append(pltpu.make_async_copy(ready.at[:, :, lanes], final.at[:, :, lanes], sem.at[len(copies)]))
        copies[-1].start()
    scale[...] = jnp.sqrt(jnp.stack([jnp.sum(jnp.swapaxes(squares[e], 0, 1), axis=0) for e in range(held)]))
    for copy in copies:
        copy.wait()


def finish(blocks, squares, routed):
    shards, held, rows, width = blocks.shape
    vmem, hbm = pl.BlockSpec(memory_space=pltpu.VMEM), pl.BlockSpec(memory_space=pl.ANY)
    return pl.pallas_call(
        finish_kernel,
        out_shape=(
            jax.ShapeDtypeStruct((held, rows, shards * width), jnp.bfloat16),
            jax.ShapeDtypeStruct((held, rows), jnp.float32),
            jax.ShapeDtypeStruct(routed.shape, jnp.bfloat16),
        ),
        in_specs=[vmem, vmem, vmem],
        out_specs=(hbm, vmem, hbm),
        scratch_shapes=[
            pltpu.VMEM((held, rows, shards * width), jnp.bfloat16),
            pltpu.VMEM((held, rows, width), jnp.float32),
            pltpu.SemaphoreType.DMA((1 + shards // GROUP,)),
        ],
        compiler_params=pltpu.CompilerParams(vmem_limit_bytes=VLIM),
    )(blocks, squares, routed)


def body(master_down, second_down, router_weight, router_gain):
    shards = lax.axis_size("shard")
    held, rows, width = master_down.shape
    cut = (held, shards, rows // shards, width)
    gathered = exchange(
        master_down.reshape(cut), second_down.reshape(cut), (router_weight.T * router_gain).astype(jnp.bfloat16), plan())
    final, scale, serve_router = finish(*gathered)
    return (final, scale, serve_router.T)


def solution(mesh):
    placed = (
        P("expert", None, "shard"),
        P("expert", None, "shard"),
        P("shard", "expert"),
        P("shard"),
    )
    return jax.shard_map(
        body,
        mesh=mesh,
        in_specs=placed,
        out_specs=(P("expert", "shard", None), P("expert", "shard"), P()),
        check_vma=False,
    )
```

```python
import functools
import jax
import jax.numpy as jnp
from jax import lax
from jax.experimental import pallas as pl
from jax.experimental.pallas import tpu as pltpu
from jax.sharding import PartitionSpec as P

MESH = pl.DeviceIdType.MESH
LONG, WIDE = 8, 4
VLIM = 50 << 20
GROUP = 4
ROUNDS = LONG // 2 + WIDE // 2 - 1
RANKED = {(LONG - 1, 0): 2.5, (LONG - 1, 1): 2, (LONG - 1, 2): 1.5}


def plan():
    early = [[(step, 0), (LONG - step, 0)] for step in range(1, LONG // 2)]
    sizes = [len(group) for group in early] + [0] * (ROUNDS - len(early))
    early = [step for group in early for step in group]
    every = [(along, across) for along in range(LONG) for across in range(WIDE) if (along, across) != (0, 0)]

    def order_at(z):
        def key(step):
            along, across = step
            target = (z + along) % LONG
            far = RANKED.get((z, target), min(along, LONG - along))
            other_half = z < LONG // 2 <= target and along != LONG // 2
            turned = (along > LONG // 2) != (across == WIDE - 1)
            return other_half, -(far + 2 * min(across, WIDE - across)), -far, turned, across, along

        return early + sorted((step for step in every if step not in early), key=key)

    orders = [order_at(z) for z in range(LONG)]
    arrivals = [sorted(every, key=lambda step: orders[(z - step[0]) % LONG].index(step)) for z in range(LONG)]
    return orders, sizes + [len(every) - len(early)], arrivals


def exchange_kernel(plan, experts, master, second, weight, gain, blocks, squares, routed,
                    router, part, scales, wide, narrow, outgoing, in_sem, send_sem, recv_sem, along_sem, across_sem, expert_sem, part_sem, round_sem):
    me, mine = lax.axis_index("shard"), lax.axis_index("expert")
    z, x = me // WIDE, lax.rem(me, WIDE)
    orders, sizes, arrivals = plan
    count = len(orders[0])

    def chosen(tables, step):
        along, across = tables[0][step]
        for place in range(1, LONG):
            along = jnp.where(z == place, tables[place][step][0], along)
            across = jnp.where(z == place, tables[place][step][1], across)
        return along, across

    def shard_at(along, across):
        return lax.rem(z + along, LONG) * WIDE + lax.rem(x + across, WIDE)

    def peer(step):
        return shard_at(*chosen(orders, step))

    def code(along, across):
        return along * WIDE + across

    def other(step):
        return lax.rem(mine + step + 1, experts)

    def greet(turn):
        semaphore = pltpu.get_barrier_semaphore() if turn == 1 else round_sem.at[turn - 2]
        for along, across in ((1, 0), (LONG - 1, 0), (0, 1), (0, WIDE - 1)):
            pl.semaphore_signal(semaphore, inc=1, device_id={"shard": shard_at(along, across)}, device_id_type=MESH)
        if turn <= 3:
            for near in around:
                pl.semaphore_signal(semaphore, inc=1, device_id={"expert": near}, device_id_type=MESH)

    def greeted(turn):
        semaphore = pltpu.get_barrier_semaphore() if turn == 1 else round_sem.at[turn - 2]
        pl.semaphore_wait(semaphore, 7 if turn <= 3 else 4)

    around = (mine + 1 - 2 * lax.rem(mine, 2), lax.rem(mine + 2, experts), lax.rem(mine + experts - 2, experts))
    def load(step):
        whom = peer(step) if step < count else me
        return (pltpu.make_async_copy(master.at[:, whom], wide.at[step], in_sem.at[step, 0]),
                pltpu.make_async_copy(second.at[:, whom], narrow.at[step], in_sem.at[step, 1]))

    def send(step, landing):
        return pltpu.make_async_remote_copy(
            src_ref=outgoing.at[step], dst_ref=blocks.at[landing], send_sem=send_sem.at[step],
            recv_sem=recv_sem.at[code(*chosen(orders, step))], device_id={"shard": peer(step)}, device_id_type=MESH)

    def arrival(step):
        along, across = chosen(arrivals, step)
        source = shard_at(LONG - along, WIDE - across)
        return source, pltpu.make_async_remote_copy(
            src_ref=outgoing.at[step], dst_ref=blocks.at[source], send_sem=send_sem.at[step],
            recv_sem=recv_sem.at[code(along, across)], device_id={"shard": source}, device_id_type=MESH)

    def merge(step):
        for copy in load(step):
            copy.wait()
        return (wide[step] + narrow[step].astype(jnp.float32)).astype(jnp.bfloat16)

    def along_copy(step, landing):
        return pltpu.make_async_remote_copy(
            src_ref=router.at[mine, z, x], dst_ref=router.at[mine, landing, x], send_sem=along_sem.at[step, 0],
            recv_sem=along_sem.at[step, 1], device_id={"shard": shard_at(step + 1, 0)}, device_id_type=MESH)

    def across_copy(step, landing):
        return pltpu.make_async_remote_copy(
            src_ref=router.at[mine, :, x], dst_ref=router.at[mine, :, landing], send_sem=across_sem.at[step, 0],
            recv_sem=across_sem.at[step, 1], device_id={"shard": shard_at(0, step + 1)}, device_id_type=MESH)

    def expert_copy(step, landing):
        return pltpu.make_async_remote_copy(
            src_ref=router.at[mine], dst_ref=router.at[landing], send_sem=expert_sem.at[step, 0],
            recv_sem=expert_sem.at[step, 1], device_id={"expert": other(step)}, device_id_type=MESH)

    def before(index, step, size):
        return lax.rem(index + size - step - 1, size)

    def loads(first, last):
        for step in range(first, last):
            for copy in load(step):
                copy.start()


    bounds = [sum(sizes[:turn]) for turn in range(ROUNDS + 2)]
    greet(1)
    loads(0, bounds[3])
    pieces = (pltpu.make_async_copy(weight, part, part_sem.at[0]), pltpu.make_async_copy(gain, scales, part_sem.at[1]))
    for copy in pieces:
        copy.start()
    for step in range(bounds[1]):
        outgoing[step] = merge(step)
    for turn in range(1, ROUNDS + 2):
        greeted(turn)
        if turn <= ROUNDS:
            greet(turn + 1)
        if turn == LONG // 2:
            for step in range(LONG - 1):
                along_copy(step, z).start()
        for step in range(bounds[turn - 1], bounds[turn]):
            send(step, me).start()
        if turn == 1:
            loads(bounds[3], count + 1)
            for copy in pieces:
                copy.wait()
            router[mine, z, x] = (part[...] * scales[...]).astype(jnp.bfloat16)
        if turn <= ROUNDS:
            for step in range(bounds[turn], bounds[turn + 1]):
                outgoing[step] = merge(step)
    for step in range(LONG - 1):
        along_copy(step, before(z, step, LONG)).wait_recv()
    for step in range(WIDE - 1):
        across_copy(step, x).start()
    own = merge(count)
    blocks[me] = own
    own = own.astype(jnp.float32)
    squares[...] = own * own
    for step in range(WIDE - 1):
        across_copy(step, before(x, step, WIDE)).wait_recv()
    for step in range(experts - 1):
        expert_copy(step, mine).start()

    for step in range(count):
        if step == count // 2:
            for turn in range(experts - 1):
                expert_copy(turn, before(mine, turn, experts)).wait_recv()
            for along in range(LONG):
                for across in range(WIDE):
                    start = (along * WIDE + across) * 128
                    routed[:, start:start + 128] = router[:, along, across].astype(jnp.float32).reshape(routed.shape[0], 128).astype(jnp.bfloat16)
        source, copy = arrival(step)
        copy.wait_recv()
        part = blocks[source].astype(jnp.float32)
        squares[...] += part * part

    for step in range(count):
        send(step, me).wait_send()
    for step in range(LONG - 1):
        along_copy(step, z).wait_send()
    for step in range(WIDE - 1):
        across_copy(step, x).wait_send()
    for step in range(experts - 1):
        expert_copy(step, mine).wait_send()


def exchange(master, second, weight, gain, plan):
    held, shards, rows, width = master.shape
    experts = lax.axis_size("expert")
    count = shards - 1
    vmem, hbm = pl.BlockSpec(memory_space=pltpu.VMEM), pl.BlockSpec(memory_space=pltpu.MemorySpace.HBM)
    dma = pltpu.SemaphoreType.DMA
    return pl.pallas_call(
        functools.partial(exchange_kernel, plan, experts),
        out_shape=(
            jax.ShapeDtypeStruct((shards, held, rows, width), jnp.bfloat16),
            jax.ShapeDtypeStruct((held, rows, width), jnp.float32),
            jax.ShapeDtypeStruct((experts * held, shards * width), jnp.bfloat16),
        ),
        in_specs=[hbm] * 4,
        out_specs=(vmem, vmem, vmem),
        scratch_shapes=[
            pltpu.VMEM((experts, LONG, WIDE, held, width), jnp.bfloat16),
            pltpu.VMEM((held, width), jnp.float32),
            pltpu.VMEM((1, width), jnp.float32),
            pltpu.VMEM((shards, held, rows, width), jnp.float32),
            pltpu.VMEM((shards, held, rows, width), jnp.bfloat16),
            pltpu.VMEM((count, held, rows, width), jnp.bfloat16),
            dma((shards, 2)), dma((count,)), dma((shards,)), dma((LONG - 1, 2)), dma((WIDE - 1, 2)),
            dma((experts - 1, 2)), dma((2,)), pltpu.SemaphoreType.REGULAR((ROUNDS,)),
        ],
        compiler_params=pltpu.CompilerParams(collective_id=0, has_side_effects=True, vmem_limit_bytes=VLIM),
    )(master, second, weight, gain)


def finish_kernel(blocks, squares, routed, final, scale, serve, ready, inverse, sem):
    held, rows, width = squares.shape
    copies = [pltpu.make_async_copy(routed, serve, sem.at[0])]
    copies[0].start()
    for e in range(held):
        inverse[e] = jnp.broadcast_to(1.0 / jnp.sqrt(jnp.sum(squares[e], axis=1, keepdims=True)), (rows, width))
    for start in range(0, blocks.shape[0], GROUP):
        for shard in range(start, start + GROUP):
            ready[:, :, shard * width:(shard + 1) * width] = (
                blocks[shard].astype(jnp.float32) * inverse[...]).astype(jnp.bfloat16)
        lanes = pl.ds(start * width, GROUP * width)
        copies.append(pltpu.make_async_copy(ready.at[:, :, lanes], final.at[:, :, lanes], sem.at[len(copies)]))
        copies[-1].start()
    scale[...] = jnp.sqrt(jnp.stack([jnp.sum(jnp.swapaxes(squares[e], 0, 1), axis=0) for e in range(held)]))
    for copy in copies:
        copy.wait()


def finish(blocks, squares, routed):
    shards, held, rows, width = blocks.shape
    vmem, hbm = pl.BlockSpec(memory_space=pltpu.VMEM), pl.BlockSpec(memory_space=pl.ANY)
    return pl.pallas_call(
        finish_kernel,
        out_shape=(
            jax.ShapeDtypeStruct((held, rows, shards * width), jnp.bfloat16),
            jax.ShapeDtypeStruct((held, rows), jnp.float32),
            jax.ShapeDtypeStruct(routed.shape, jnp.bfloat16),
        ),
        in_specs=[vmem, vmem, vmem],
        out_specs=(hbm, vmem, hbm),
        scratch_shapes=[
            pltpu.VMEM((held, rows, shards * width), jnp.bfloat16),
            pltpu.VMEM((held, rows, width), jnp.float32),
            pltpu.SemaphoreType.DMA((1 + shards // GROUP,)),
        ],
        compiler_params=pltpu.CompilerParams(vmem_limit_bytes=VLIM),
    )(blocks, squares, routed)


def body(master_down, second_down, router_weight, router_gain):
    shards = lax.axis_size("shard")
    held, rows, width = master_down.shape
    cut = (held, shards, rows // shards, width)
    gathered = exchange(
        *(pltpu.with_memory_space_constraint(value, pltpu.HBM) for value in (
            master_down.reshape(cut), second_down.reshape(cut), router_weight.T, router_gain[None, :])), plan())
    final, scale, serve_router = finish(*gathered)
    return (final, scale, serve_router.T)


def solution(mesh):
    placed = (
        P("expert", None, "shard"),
        P("expert", None, "shard"),
        P("shard", "expert"),
        P("shard"),
    )
    return jax.shard_map(
        body,
        mesh=mesh,
        in_specs=placed,
        out_specs=(P("expert", "shard", None), P("expert", "shard"), P()),
        check_vma=False,
    )
```

```python
import functools
import jax
import jax.numpy as jnp
from jax import lax
from jax.experimental import pallas as pl
from jax.experimental.pallas import tpu as pltpu
from jax.sharding import PartitionSpec as P

MESH = pl.DeviceIdType.MESH
LONG, WIDE = 8, 4
VLIM = 50 << 20
CUT = 40
ROUNDS = LONG // 2 + WIDE // 2 - 1
RANKED = {(LONG - 1, 0): 2.5, (LONG - 1, 1): 2, (LONG - 1, 2): 1.5}


def plan():
    early = [[(step, 0), (LONG - step, 0)] for step in range(1, LONG // 2)]
    sizes = [len(group) for group in early] + [0] * (ROUNDS - len(early))
    early = [step for group in early for step in group]
    every = [(along, across) for along in range(LONG) for across in range(WIDE) if (along, across) != (0, 0)]

    def order_at(z):
        def key(step):
            along, across = step
            target = (z + along) % LONG
            far = RANKED.get((z, target), min(along, LONG - along))
            other_half = z < LONG // 2 <= target and along != LONG // 2
            turned = (along > LONG // 2) != (across == WIDE - 1)
            return other_half, -(far + 2 * min(across, WIDE - across)), -far, turned, across, along

        return early + sorted((step for step in every if step not in early), key=key)

    orders = [order_at(z) for z in range(LONG)]
    arrivals = [sorted(every, key=lambda step: orders[(z - step[0]) % LONG].index(step)) for z in range(LONG)]
    return orders, sizes + [len(every) - len(early)], arrivals


def exchange_kernel(plan, experts, master, second, weight, gain, blocks, squares, routed,
                    router, part, scales, wide, narrow, outgoing, in_sem, send_sem, recv_sem, along_sem, across_sem, expert_sem, part_sem, round_sem):
    me, mine = lax.axis_index("shard"), lax.axis_index("expert")
    z, x = me // WIDE, lax.rem(me, WIDE)
    orders, sizes, arrivals = plan
    count = len(orders[0])

    def chosen(tables, step):
        along, across = tables[0][step]
        for place in range(1, LONG):
            along = jnp.where(z == place, tables[place][step][0], along)
            across = jnp.where(z == place, tables[place][step][1], across)
        return along, across

    def shard_at(along, across):
        return lax.rem(z + along, LONG) * WIDE + lax.rem(x + across, WIDE)

    def peer(step):
        return shard_at(*chosen(orders, step))

    def code(along, across):
        return along * WIDE + across

    def other(step):
        return lax.rem(mine + step + 1, experts)

    def greet(turn):
        semaphore = pltpu.get_barrier_semaphore() if turn == 1 else round_sem.at[turn - 2]
        for along, across in ((1, 0), (LONG - 1, 0), (0, 1), (0, WIDE - 1)):
            pl.semaphore_signal(semaphore, inc=1, device_id={"shard": shard_at(along, across)}, device_id_type=MESH)
        if turn <= 3:
            for near in around:
                pl.semaphore_signal(semaphore, inc=1, device_id={"expert": near}, device_id_type=MESH)

    def greeted(turn):
        semaphore = pltpu.get_barrier_semaphore() if turn == 1 else round_sem.at[turn - 2]
        pl.semaphore_wait(semaphore, 7 if turn <= 3 else 4)

    around = (mine + 1 - 2 * lax.rem(mine, 2), lax.rem(mine + 2, experts), lax.rem(mine + experts - 2, experts))
    def load(step):
        whom = peer(step) if step < count else me
        return (pltpu.make_async_copy(master.at[:, whom], wide.at[step], in_sem.at[step, 0]),
                pltpu.make_async_copy(second.at[:, whom], narrow.at[step], in_sem.at[step, 1]))

    def send(step, landing):
        return pltpu.make_async_remote_copy(
            src_ref=outgoing.at[step], dst_ref=blocks.at[landing], send_sem=send_sem.at[step],
            recv_sem=recv_sem.at[code(*chosen(orders, step))], device_id={"shard": peer(step)}, device_id_type=MESH)

    def arrival(step):
        along, across = chosen(arrivals, step)
        source = shard_at(LONG - along, WIDE - across)
        return source, pltpu.make_async_remote_copy(
            src_ref=outgoing.at[step], dst_ref=blocks.at[source], send_sem=send_sem.at[step],
            recv_sem=recv_sem.at[code(along, across)], device_id={"shard": source}, device_id_type=MESH)

    def merge(step):
        for copy in load(step):
            copy.wait()
        return (wide[step] + narrow[step].astype(jnp.float32)).astype(jnp.bfloat16)

    def along_copy(step, landing):
        return pltpu.make_async_remote_copy(
            src_ref=router.at[mine, z, x], dst_ref=router.at[mine, landing, x], send_sem=along_sem.at[step, 0],
            recv_sem=along_sem.at[step, 1], device_id={"shard": shard_at(step + 1, 0)}, device_id_type=MESH)

    def across_copy(step, landing):
        return pltpu.make_async_remote_copy(
            src_ref=router.at[mine, :, x], dst_ref=router.at[mine, :, landing], send_sem=across_sem.at[step, 0],
            recv_sem=across_sem.at[step, 1], device_id={"shard": shard_at(0, step + 1)}, device_id_type=MESH)

    def expert_copy(step, landing):
        return pltpu.make_async_remote_copy(
            src_ref=router.at[mine], dst_ref=router.at[landing], send_sem=expert_sem.at[step, 0],
            recv_sem=expert_sem.at[step, 1], device_id={"expert": other(step)}, device_id_type=MESH)

    def before(index, step, size):
        return lax.rem(index + size - step - 1, size)

    def loads(first, last):
        for step in range(first, last):
            for copy in load(step):
                copy.start()


    bounds = [sum(sizes[:turn]) for turn in range(ROUNDS + 2)]
    greet(1)
    loads(0, bounds[3])
    pieces = (pltpu.make_async_copy(weight, part, part_sem.at[0]), pltpu.make_async_copy(gain, scales, part_sem.at[1]))
    for copy in pieces:
        copy.start()
    for step in range(bounds[1]):
        outgoing[step] = merge(step)
    for turn in range(1, ROUNDS + 2):
        greeted(turn)
        if turn <= ROUNDS:
            greet(turn + 1)
        if turn == LONG // 2:
            for step in range(LONG - 1):
                along_copy(step, z).start()
        for step in range(bounds[turn - 1], bounds[turn]):
            send(step, me).start()
        if turn == 1:
            loads(bounds[3], count + 1)
            for copy in pieces:
                copy.wait()
            router[mine, z, x] = (part[...] * scales[...]).astype(jnp.bfloat16)
        if turn <= ROUNDS:
            for step in range(bounds[turn], bounds[turn + 1]):
                outgoing[step] = merge(step)
    for step in range(LONG - 1):
        along_copy(step, before(z, step, LONG)).wait_recv()
    for step in range(WIDE - 1):
        across_copy(step, x).start()
    own = merge(count)
    blocks[me] = own
    own = own.astype(jnp.float32)
    squares[...] = own * own
    for step in range(WIDE - 1):
        across_copy(step, before(x, step, WIDE)).wait_recv()
    for step in range(experts - 1):
        expert_copy(step, mine).start()

    for step in range(count):
        if step == count // 2:
            for turn in range(experts - 1):
                expert_copy(turn, before(mine, turn, experts)).wait_recv()
            for along in range(LONG):
                for across in range(WIDE):
                    start = (along * WIDE + across) * 128
                    routed[:, start:start + 128] = router[:, along, across].astype(jnp.float32).reshape(routed.shape[0], 128).astype(jnp.bfloat16)
        source, copy = arrival(step)
        copy.wait_recv()
        part = blocks[source].astype(jnp.float32)
        squares[...] += part * part

    for step in range(count):
        send(step, me).wait_send()
    for step in range(LONG - 1):
        along_copy(step, z).wait_send()
    for step in range(WIDE - 1):
        across_copy(step, x).wait_send()
    for step in range(experts - 1):
        expert_copy(step, mine).wait_send()


def exchange(master, second, weight, gain, plan):
    held, shards, rows, width = master.shape
    experts = lax.axis_size("expert")
    count = shards - 1
    vmem, hbm = pl.BlockSpec(memory_space=pltpu.VMEM), pl.BlockSpec(memory_space=pltpu.MemorySpace.HBM)
    dma = pltpu.SemaphoreType.DMA
    return pl.pallas_call(
        functools.partial(exchange_kernel, plan, experts),
        out_shape=(
            jax.ShapeDtypeStruct((shards, held, rows, width), jnp.bfloat16),
            jax.ShapeDtypeStruct((held, rows, width), jnp.float32),
            jax.ShapeDtypeStruct((experts * held, shards * width), jnp.bfloat16),
        ),
        in_specs=[hbm] * 4,
        out_specs=(vmem, vmem, vmem),
        scratch_shapes=[
            pltpu.VMEM((experts, LONG, WIDE, held, width), jnp.bfloat16),
            pltpu.VMEM((held, width), jnp.float32),
            pltpu.VMEM((1, width), jnp.float32),
            pltpu.VMEM((shards, held, rows, width), jnp.float32),
            pltpu.VMEM((shards, held, rows, width), jnp.bfloat16),
            pltpu.VMEM((count, held, rows, width), jnp.bfloat16),
            dma((shards, 2)), dma((count,)), dma((shards,)), dma((LONG - 1, 2)), dma((WIDE - 1, 2)),
            dma((experts - 1, 2)), dma((2,)), pltpu.SemaphoreType.REGULAR((ROUNDS,)),
        ],
        compiler_params=pltpu.CompilerParams(collective_id=0, has_side_effects=True, vmem_limit_bytes=VLIM),
    )(master, second, weight, gain)


def finish_kernel(blocks, squares, routed, final, scale, serve, ready, root, sem):
    held, rows, width = squares.shape
    copies = [pltpu.make_async_copy(routed, serve, sem.at[0])]
    copies[0].start()
    for start in range(0, rows, CUT):
        part = pl.ds(start, CUT)
        total = jnp.sum(squares[:, part], axis=2, keepdims=True)
        inverse = jnp.broadcast_to(1.0 / jnp.sqrt(total), (held, CUT, width))
        for shard in range(blocks.shape[0]):
            ready[:, part, shard * width:(shard + 1) * width] = (
                blocks[shard, :, part].astype(jnp.float32) * inverse).astype(jnp.bfloat16)
        copies.append(pltpu.make_async_copy(ready.at[:, part], final.at[:, part], sem.at[len(copies)]))
        copies[-1].start()
    root[...] = jnp.sqrt(jnp.stack([jnp.sum(jnp.swapaxes(squares[e], 0, 1), axis=0) for e in range(held)]))
    copies.append(pltpu.make_async_copy(root, scale, sem.at[len(copies)]))
    copies[-1].start()
    for copy in copies:
        copy.wait()


def finish(blocks, squares, routed):
    shards, held, rows, width = blocks.shape
    vmem, hbm = pl.BlockSpec(memory_space=pltpu.VMEM), pl.BlockSpec(memory_space=pl.ANY)
    return pl.pallas_call(
        finish_kernel,
        out_shape=(
            jax.ShapeDtypeStruct((held, rows, shards * width), jnp.bfloat16),
            jax.ShapeDtypeStruct((held, rows), jnp.float32),
            jax.ShapeDtypeStruct(routed.shape, jnp.bfloat16),
        ),
        in_specs=[vmem, vmem, vmem],
        out_specs=(hbm, hbm, hbm),
        scratch_shapes=[
            pltpu.VMEM((held, rows, shards * width), jnp.bfloat16),
            pltpu.VMEM((held, rows), jnp.float32),
            pltpu.SemaphoreType.DMA((2 + rows // CUT,)),
        ],
        compiler_params=pltpu.CompilerParams(vmem_limit_bytes=VLIM),
    )(blocks, squares, routed)


def body(master_down, second_down, router_weight, router_gain):
    shards = lax.axis_size("shard")
    held, rows, width = master_down.shape
    cut = (held, shards, rows // shards, width)
    gathered = exchange(
        *(pltpu.with_memory_space_constraint(value, pltpu.HBM) for value in (
            master_down.reshape(cut), second_down.reshape(cut), router_weight.T, router_gain[None, :])), plan())
    final, scale, serve_router = finish(*gathered)
    return (final, scale, serve_router.T)


def solution(mesh):
    placed = (
        P("expert", None, "shard"),
        P("expert", None, "shard"),
        P("shard", "expert"),
        P("shard"),
    )
    return jax.shard_map(
        body,
        mesh=mesh,
        in_specs=placed,
        out_specs=(P("expert", "shard", None), P("expert", "shard"), P()),
        check_vma=False,
    )
```

```python
import functools
import jax
import jax.numpy as jnp
from jax import lax
from jax.experimental import pallas as pl
from jax.experimental.pallas import tpu as pltpu
from jax.sharding import PartitionSpec as P

MESH = pl.DeviceIdType.MESH
LONG, WIDE = 8, 4
VLIM = 50 << 20
CUT = 40
FIRST = 8
ROUNDS = LONG // 2 + WIDE // 2 - 1
RANKED = {(LONG - 1, 0): 2.5, (LONG - 1, 1): 2, (LONG - 1, 2): 1.5}


def plan():
    early = [[(step, 0), (LONG - step, 0)] for step in range(1, LONG // 2)]
    sizes = [len(group) for group in early] + [0] * (ROUNDS - len(early))
    early = [step for group in early for step in group]
    every = [(along, across) for along in range(LONG) for across in range(WIDE) if (along, across) != (0, 0)]

    def order_at(z):
        def key(step):
            along, across = step
            target = (z + along) % LONG
            far = RANKED.get((z, target), min(along, LONG - along))
            other_half = z < LONG // 2 <= target and along != LONG // 2
            turned = (along > LONG // 2) != (across == WIDE - 1)
            return other_half, -(far + 1.75 * min(across, WIDE - across)), -far, turned, across, along

        return early + sorted((step for step in every if step not in early), key=key)

    orders = [order_at(z) for z in range(LONG)]
    arrivals = [sorted(every, key=lambda step: orders[(z - step[0]) % LONG].index(step)) for z in range(LONG)]
    return orders, sizes + [len(every) - len(early)], arrivals


def exchange_kernel(plan, experts, master, second, weight, gain, blocks, squares, routed,
                    router, part, scales, wide, narrow, outgoing, in_sem, send_sem, recv_sem, along_sem, across_sem, expert_sem, part_sem, round_sem):
    me, mine = lax.axis_index("shard"), lax.axis_index("expert")
    z, x = me // WIDE, lax.rem(me, WIDE)
    orders, sizes, arrivals = plan
    count = len(orders[0])

    def chosen(tables, step):
        along, across = tables[0][step]
        for place in range(1, LONG):
            along = jnp.where(z == place, tables[place][step][0], along)
            across = jnp.where(z == place, tables[place][step][1], across)
        return along, across

    def shard_at(along, across):
        return lax.rem(z + along, LONG) * WIDE + lax.rem(x + across, WIDE)

    def peer(step):
        return shard_at(*chosen(orders, step))

    def code(along, across):
        return along * WIDE + across

    def other(step):
        return lax.rem(mine + step + 1, experts)

    def greet(turn):
        semaphore = pltpu.get_barrier_semaphore() if turn == 1 else round_sem.at[turn - 2]
        for along, across in ((1, 0), (LONG - 1, 0), (0, 1), (0, WIDE - 1)):
            pl.semaphore_signal(semaphore, inc=1, device_id={"shard": shard_at(along, across)}, device_id_type=MESH)
        if turn <= 3:
            for near in around:
                pl.semaphore_signal(semaphore, inc=1, device_id={"expert": near}, device_id_type=MESH)

    def greeted(turn):
        semaphore = pltpu.get_barrier_semaphore() if turn == 1 else round_sem.at[turn - 2]
        pl.semaphore_wait(semaphore, 7 if turn <= 3 else 4)

    around = (mine + 1 - 2 * lax.rem(mine, 2), lax.rem(mine + 2, experts), lax.rem(mine + experts - 2, experts))
    def load(step):
        whom = peer(step) if step < count else me
        return (pltpu.make_async_copy(master.at[:, whom], wide.at[step], in_sem.at[step, 0]),
                pltpu.make_async_copy(second.at[:, whom], narrow.at[step], in_sem.at[step, 1]))

    def send(step, landing):
        return pltpu.make_async_remote_copy(
            src_ref=outgoing.at[step], dst_ref=blocks.at[landing], send_sem=send_sem.at[step],
            recv_sem=recv_sem.at[code(*chosen(orders, step))], device_id={"shard": peer(step)}, device_id_type=MESH)

    def arrival(step):
        along, across = chosen(arrivals, step)
        source = shard_at(LONG - along, WIDE - across)
        return source, pltpu.make_async_remote_copy(
            src_ref=outgoing.at[step], dst_ref=blocks.at[source], send_sem=send_sem.at[step],
            recv_sem=recv_sem.at[code(along, across)], device_id={"shard": source}, device_id_type=MESH)

    def merge(step):
        for copy in load(step):
            copy.wait()
        return (wide[step] + narrow[step].astype(jnp.float32)).astype(jnp.bfloat16)

    def along_copy(step, landing):
        return pltpu.make_async_remote_copy(
            src_ref=router.at[mine, z, x], dst_ref=router.at[mine, landing, x], send_sem=along_sem.at[step, 0],
            recv_sem=along_sem.at[step, 1], device_id={"shard": shard_at(step + 1, 0)}, device_id_type=MESH)

    def across_copy(step, landing):
        return pltpu.make_async_remote_copy(
            src_ref=router.at[mine, :, x], dst_ref=router.at[mine, :, landing], send_sem=across_sem.at[step, 0],
            recv_sem=across_sem.at[step, 1], device_id={"shard": shard_at(0, step + 1)}, device_id_type=MESH)

    def expert_copy(step, landing):
        return pltpu.make_async_remote_copy(
            src_ref=router.at[mine], dst_ref=router.at[landing], send_sem=expert_sem.at[step, 0],
            recv_sem=expert_sem.at[step, 1], device_id={"expert": other(step)}, device_id_type=MESH)

    def before(index, step, size):
        return lax.rem(index + size - step - 1, size)

    def loads(first, last):
        for step in range(first, last):
            for copy in load(step):
                copy.start()


    bounds = [sum(sizes[:turn]) for turn in range(ROUNDS + 2)]
    greet(1)
    loads(0, bounds[3])
    pieces = (pltpu.make_async_copy(weight, part, part_sem.at[0]), pltpu.make_async_copy(gain, scales, part_sem.at[1]))
    for copy in pieces:
        copy.start()
    for step in range(bounds[1]):
        outgoing[step] = merge(step)
    for turn in range(1, ROUNDS + 2):
        greeted(turn)
        if turn <= ROUNDS:
            greet(turn + 1)
        if turn == LONG // 2:
            for step in range(LONG - 1):
                along_copy(step, z).start()
        for step in range(bounds[turn - 1], bounds[turn]):
            send(step, me).start()
        if turn == 1:
            loads(bounds[3], count + 1)
            for copy in pieces:
                copy.wait()
            router[mine, z, x] = (part[...] * scales[...]).astype(jnp.bfloat16)
        if turn <= ROUNDS:
            for step in range(bounds[turn], bounds[turn + 1]):
                outgoing[step] = merge(step)
    for step in range(LONG - 1):
        along_copy(step, before(z, step, LONG)).wait_recv()
    for step in range(WIDE - 1):
        across_copy(step, x).start()
    own = merge(count)
    blocks[me] = own
    own = own.astype(jnp.float32)
    squares[...] = own * own
    for step in range(WIDE - 1):
        across_copy(step, before(x, step, WIDE)).wait_recv()
    for step in range(experts - 1):
        expert_copy(step, mine).start()

    for step in range(count):
        if step == count // 2:
            for turn in range(experts - 1):
                expert_copy(turn, before(mine, turn, experts)).wait_recv()
            for along in range(LONG):
                for across in range(WIDE):
                    start = (along * WIDE + across) * 128
                    routed[:, start:start + 128] = router[:, along, across].astype(jnp.float32).reshape(routed.shape[0], 128).astype(jnp.bfloat16)
        source, copy = arrival(step)
        copy.wait_recv()
        part = blocks[source].astype(jnp.float32)
        squares[...] += part * part

    for step in range(count):
        send(step, me).wait_send()
    for step in range(LONG - 1):
        along_copy(step, z).wait_send()
    for step in range(WIDE - 1):
        across_copy(step, x).wait_send()
    for step in range(experts - 1):
        expert_copy(step, mine).wait_send()


def exchange(master, second, weight, gain, plan):
    held, shards, rows, width = master.shape
    experts = lax.axis_size("expert")
    count = shards - 1
    vmem, hbm = pl.BlockSpec(memory_space=pltpu.VMEM), pl.BlockSpec(memory_space=pltpu.MemorySpace.HBM)
    dma = pltpu.SemaphoreType.DMA
    return pl.pallas_call(
        functools.partial(exchange_kernel, plan, experts),
        out_shape=(
            jax.ShapeDtypeStruct((shards, held, rows, width), jnp.bfloat16),
            jax.ShapeDtypeStruct((held, rows, width), jnp.float32),
            jax.ShapeDtypeStruct((experts * held, shards * width), jnp.bfloat16),
        ),
        in_specs=[hbm] * 4,
        out_specs=(vmem, vmem, vmem),
        scratch_shapes=[
            pltpu.VMEM((experts, LONG, WIDE, held, width), jnp.bfloat16),
            pltpu.VMEM((held, width), jnp.float32),
            pltpu.VMEM((1, width), jnp.float32),
            pltpu.VMEM((shards, held, rows, width), jnp.float32),
            pltpu.VMEM((shards, held, rows, width), jnp.bfloat16),
            pltpu.VMEM((count, held, rows, width), jnp.bfloat16),
            dma((shards, 2)), dma((count,)), dma((shards,)), dma((LONG - 1, 2)), dma((WIDE - 1, 2)),
            dma((experts - 1, 2)), dma((2,)), pltpu.SemaphoreType.REGULAR((ROUNDS,)),
        ],
        compiler_params=pltpu.CompilerParams(collective_id=0, has_side_effects=True, vmem_limit_bytes=VLIM),
    )(master, second, weight, gain)


def finish_kernel(blocks, squares, routed, final, scale, serve, ready, root, sem):
    held, rows, width = squares.shape
    copies = [pltpu.make_async_copy(routed, serve, sem.at[0])]
    copies[0].start()
    for start, size in [(0, FIRST), (FIRST, CUT - FIRST)] + [(start, CUT) for start in range(CUT, rows, CUT)]:
        part = pl.ds(start, size)
        total = jnp.sum(squares[:, part], axis=2, keepdims=True)
        inverse = jnp.broadcast_to(1.0 / jnp.sqrt(total), (held, size, width))
        for shard in range(blocks.shape[0]):
            ready[:, part, shard * width:(shard + 1) * width] = (
                blocks[shard, :, part].astype(jnp.float32) * inverse).astype(jnp.bfloat16)
        copies.append(pltpu.make_async_copy(ready.at[:, part], final.at[:, part], sem.at[len(copies)]))
        copies[-1].start()
    root[...] = jnp.sqrt(jnp.stack([jnp.sum(jnp.swapaxes(squares[e], 0, 1), axis=0) for e in range(held)]))
    copies.append(pltpu.make_async_copy(root, scale, sem.at[len(copies)]))
    copies[-1].start()
    for copy in copies:
        copy.wait()


def finish(blocks, squares, routed):
    shards, held, rows, width = blocks.shape
    vmem, hbm = pl.BlockSpec(memory_space=pltpu.VMEM), pl.BlockSpec(memory_space=pl.ANY)
    return pl.pallas_call(
        finish_kernel,
        out_shape=(
            jax.ShapeDtypeStruct((held, rows, shards * width), jnp.bfloat16),
            jax.ShapeDtypeStruct((held, rows), jnp.float32),
            jax.ShapeDtypeStruct(routed.shape, jnp.bfloat16),
        ),
        in_specs=[vmem, vmem, vmem],
        out_specs=(hbm, hbm, hbm),
        scratch_shapes=[
            pltpu.VMEM((held, rows, shards * width), jnp.bfloat16),
            pltpu.VMEM((held, rows), jnp.float32),
            pltpu.SemaphoreType.DMA((3 + rows // CUT,)),
        ],
        compiler_params=pltpu.CompilerParams(vmem_limit_bytes=VLIM),
    )(blocks, squares, routed)


def body(master_down, second_down, router_weight, router_gain):
    shards = lax.axis_size("shard")
    held, rows, width = master_down.shape
    cut = (held, shards, rows // shards, width)
    gathered = exchange(
        *(pltpu.with_memory_space_constraint(value, pltpu.HBM) for value in (
            master_down.reshape(cut), second_down.reshape(cut), router_weight.T, router_gain[None, :])), plan())
    final, scale, serve_router = finish(*gathered)
    return (final, scale, serve_router.T)


def solution(mesh):
    placed = (
        P("expert", None, "shard"),
        P("expert", None, "shard"),
        P("shard", "expert"),
        P("shard"),
    )
    return jax.shard_map(
        body,
        mesh=mesh,
        in_specs=placed,
        out_specs=(P("expert", "shard", None), P("expert", "shard"), P()),
        check_vma=False,
    )
```
